32 devices in a mesh: batch: 4 (over x, core), row: 2 (over y), col: 4 (over z).
Axes of the slice: x: 2, y: 2, z: 4, core: 2. Of those that a mesh axis runs over, the one named last changes fastest.
Arguments:
- inputs: float32 [8192, 1536], P(('batch', 'col'), 'row'), may hold values from -8 to 8
- segments: int32 [16, 512], P(('batch', 'row')), may hold values from 0 to 511, as said below
- positions: int32 [16, 512], P(('batch', 'row')), may hold values from 0 to 2558, as said below
- gain_attn: float32 [1536], P('row'), may hold values from 0.5 to 1.5
- gain_mlp: float32 [1536], P('row'), may hold values from 0.5 to 1.5
- w_qkv: bfloat16 [1536, 1536], P('row', 'col'), may hold values from -0.19385052 to 0.19385052
- w_out: bfloat16 [768, 1536], P('col', 'row'), may hold values from -1.25 to 1.25
- w_gate: bfloat16 [1536, 4096], P('row', 'col'), may hold values from -0.15625 to 0.15625
- w_up: bfloat16 [1536, 4096], P('row', 'col'), may hold values from -0.15625 to 0.15625
- w_down: bfloat16 [4096, 1536], P('col', 'row'), may hold values from -0.09375 to 0.09375
- grad_output: float32 [8192, 1536], P(('batch', 'col'), 'row'), may hold values from -6 to 6
Outputs:
- result: float32 [8192, 1536], P(('batch', 'col'), 'row')
- grad_inputs: float32 [8192, 1536], P(('batch', 'col'), 'row')
- grad_gain_attn: float32 [1536], P('row')
- grad_gain_mlp: float32 [1536], P('row')
- grad_w_qkv: float32 [1536, 1536], P('row', 'col')
- grad_w_out: float32 [768, 1536], P('col', 'row')
- grad_w_gate: float32 [1536, 4096], P('row', 'col')
- grad_w_up: float32 [1536, 4096], P('row', 'col')
- grad_w_down: float32 [4096, 1536], P('col', 'row')
The draws below stay inside these ranges and needn't reach their ends.
Inputs may be any that keep to these rules, and one draw needn't show every extreme that they name: `segments`: in each packed row the segment numbers start at 0 and never fall. `positions`: inside a segment the position rises by one from token to token.
All inputs are finite; a program needn't handle non-finite values.
Results may differ from the reference program's by a relative error of at most 0.015.
The reference program's roundings to bfloat16 on the way count: a program that leaves them out, or rounds other values in their place, can miss the bound.
Values may be sent and summed in bfloat16 or wider, within the bound.
A program may use at most 192 MiB of HBM per device.

```python
import jax
import jax.numpy as jnp
from jax import lax

D = 1536
HD = 96
FF = 4096
HQ_DEV = 2
KV = 4
HEADS = 8
SEQ = 512
ROWS = 16
TOKENS = 8192


def segment_plan(key):
    plan_key = jax.random.fold_in(key, 7)
    column_index = jnp.arange(SEQ, dtype=jnp.int32)
    row_index = jnp.arange(ROWS, dtype=jnp.int32)
    breaks = jax.random.randint(plan_key, (ROWS, SEQ), 0, 48) == 0
    breaks = breaks | (column_index == 0)[None, :]
    breaks = breaks | (row_index == 0)[:, None]
    breaks = jnp.where((row_index == 1)[:, None], (column_index == 0)[None, :], breaks)
    seg_ids = jnp.cumsum(breaks.astype(jnp.int32), axis=1) - 1
    starts = lax.cummax(jnp.where(breaks, column_index[None, :], 0), axis=1)
    offsets = jax.random.randint(jax.random.fold_in(key, 11), (ROWS, SEQ), 0, 2048)
    first_cell = (row_index[:, None] < 2) & (column_index[None, :] == 0)
    offsets = jnp.where(first_cell, jnp.where(row_index[:, None] == 0, 0, 2047), offsets)
    position_vals = column_index[None, :] - starts + jnp.take_along_axis(offsets, starts, axis=1)
    return (seg_ids.astype(jnp.int32), position_vals.astype(jnp.int32))


def draw_segments(key, part):
    return segment_plan(key)[0]


def draw_positions(key, part):
    return segment_plan(key)[1]


def draw_inputs(key, part):
    noise_key = jax.random.fold_in(key, 201)
    values = jnp.clip(jax.random.normal(noise_key, (TOKENS, D), jnp.float32), -6.0, 6.0)
    return values


def draw_w_qkv(key, part):
    width_all = KV * (HQ_DEV + 2) * HD
    noise_key = jax.random.fold_in(key, 301)
    values = jnp.clip(jax.random.normal(noise_key, (D, width_all), jnp.float32), -6.0, 6.0) * D ** (-0.5)
    return values.astype(jnp.bfloat16)


def level_of(key, shape, cuts, least, top_value):
    level, own = 1.0, jax.random.fold_in(key, 6)
    for dim, blocks in cuts:
        steps = jnp.exp(jax.random.uniform(jax.random.fold_in(own, dim), (blocks,), jnp.float32, least / len(cuts), top_value / len(cuts)))
        level = level * jnp.repeat(steps, shape[dim] // blocks).reshape([-1 if axis == dim else 1 for axis in range(len(shape))])
    return level


def bell_draw(stream_key, dims, width, reach, shards=(), held_as=jnp.bfloat16):
    entries = jax.random.normal(stream_key, dims, jnp.float32) * width
    if len(shards) > 0:
        entries = level_of(stream_key, dims, shards, -0.22, 0.18) * entries
    return jnp.clip(entries, min=-reach, max=reach).astype(held_as)


def setup_inputs(seed: int = 0) -> dict:
    key_list = jax.random.split(jax.random.key(seed), 12)
    inputs = draw_inputs(jax.random.fold_in(key_list[11], 71), 0)
    segments = draw_segments(jax.random.fold_in(key_list[11], 71), 0)
    positions = draw_positions(jax.random.fold_in(key_list[11], 71), 0)
    gain_attn = jnp.clip(1.0 + 0.1 * jax.random.normal(key_list[3], (D,), jnp.float32), 0.5, 1.5)
    gain_mlp = jnp.clip(1.0 + 0.1 * jax.random.normal(key_list[4], (D,), jnp.float32), 0.5, 1.5)
    w_qkv = draw_w_qkv(jax.random.fold_in(key_list[11], 71), 0)
    w_out = bell_draw(key_list[6], (HEADS * HD, D), (HEADS * HD // 32) ** -0.5, 1.25, ((0, 4), (1, 2)))
    w_gate = bell_draw(key_list[7], (D, FF), D ** -0.5, 0.15625, ((0, 2), (1, 4)))
    w_up = bell_draw(key_list[8], (D, FF), D ** -0.5, 0.15625, ((0, 2), (1, 4)))
    w_down = bell_draw(key_list[9], (FF, D), FF ** -0.5, 0.09375, ((0, 4), (1, 2)))
    grad_output = bell_draw(key_list[10], (TOKENS, D), 1.0, 6.0, ((0, 16), (1, 2)), jnp.float32)
    return {"inputs": inputs, "segments": segments, "positions": positions, "gain_attn": gain_attn, "gain_mlp": gain_mlp, "w_qkv": w_qkv, "w_out": w_out, "w_gate": w_gate, "w_up": w_up, "w_down": w_down, "grad_output": grad_output}


EPS = 1e-05
ROPE_BASE = 100000.0
NEG_FILL = -1e+30

def rms_forward(values, gain_vec):
    inverse = lax.rsqrt(lax.optimization_barrier(jnp.mean(values * values, axis=-1, keepdims=True)) + EPS)
    normed = values * inverse
    return (normed, inverse, (normed * gain_vec).astype(jnp.bfloat16))

def rms_backward(upstream, grad_hidden, normed, inverse, gain_vec):
    scaled = grad_hidden * gain_vec
    centre = lax.optimization_barrier(jnp.mean(scaled * normed, axis=-1, keepdims=True))
    return (upstream + inverse * (scaled - normed * centre), lax.optimization_barrier(jnp.sum(grad_hidden * normed, axis=0)))

def rope_tables(positions, head_size):
    half_size = head_size // 2
    frequency = ROPE_BASE ** (-(jnp.arange(half_size, dtype=jnp.float32) * 2.0 / head_size))
    angles = positions.astype(jnp.float32)[..., None] * frequency
    return (jnp.cos(angles), jnp.sin(angles))

def rotate(tensor, cosine_table, sine_table):
    half_size = tensor.shape[-1] // 2
    front_half = tensor[..., :half_size]
    back_half = tensor[..., half_size:]
    return jnp.concatenate([front_half * cosine_table - back_half * sine_table, back_half * cosine_table + front_half * sine_table], axis=-1)

def masked_scores(query_row, key_row, seg_row):
    scores = jnp.einsum('qghd,kgd->ghqk', query_row.astype(jnp.float32), key_row.astype(jnp.float32)) / jnp.sqrt(jnp.float32(HD))
    order = jnp.arange(SEQ)
    allowed = (seg_row[:, None] == seg_row[None, :]) & (order[:, None] >= order[None, :])
    return jnp.where(allowed[None, None], scores, NEG_FILL)

def attend_row(packed):
    query_row, key_row, value_row, seg_row = packed
    scores = masked_scores(query_row, key_row, seg_row)
    row_max = lax.optimization_barrier(jnp.max(scores, axis=-1, keepdims=True))
    log_total = row_max + jnp.log(lax.optimization_barrier(jnp.sum(jnp.exp(scores - row_max), axis=-1, keepdims=True)))
    probs_b = jnp.exp(scores - log_total).astype(jnp.bfloat16)
    probs_b = lax.optimization_barrier(probs_b)
    attention_output = jnp.einsum('ghqk,kgd->qghd', probs_b.astype(jnp.float32), value_row.astype(jnp.float32))
    return (attention_output.astype(jnp.bfloat16), log_total)

def attend_back_row(packed):
    query_row, key_row, value_row, seg_row, log_total, grad_row = packed
    scores = masked_scores(query_row, key_row, seg_row)
    weights_f = jnp.exp(scores - log_total)
    grad_probs = jnp.einsum('qghd,kgd->ghqk', grad_row.astype(jnp.float32), value_row.astype(jnp.float32))
    centre = lax.optimization_barrier(jnp.sum(weights_f * grad_probs, axis=-1, keepdims=True))
    score_gradient = (weights_f * (grad_probs - centre)).astype(jnp.bfloat16)
    score_gradient = lax.optimization_barrier(score_gradient).astype(jnp.float32)
    attention_weight_matrix = lax.optimization_barrier(weights_f.astype(jnp.bfloat16)).astype(jnp.float32)
    score_scale = 1.0 / jnp.sqrt(jnp.float32(HD))
    grad_qrot = jnp.einsum('ghqk,kgd->qghd', score_gradient, key_row.astype(jnp.float32)) * score_scale
    grad_krot = jnp.einsum('ghqk,qghd->kgd', score_gradient, query_row.astype(jnp.float32)) * score_scale
    grad_value = jnp.einsum('ghqk,qghd->kgd', attention_weight_matrix, grad_row.astype(jnp.float32))
    return (grad_qrot, grad_krot, grad_value)

def tdot(left, right):
    return jnp.dot(left.T, right, preferred_element_type=jnp.float32)

def reference(inputs, segments, positions, gain_attn, gain_mlp, w_qkv, w_out, w_gate, w_up, w_down, grad_output):
    bf = jnp.bfloat16
    normed_one, inverse_one, hidden_one = rms_forward(inputs, gain_attn)
    projected = jnp.dot(hidden_one, w_qkv, preferred_element_type=jnp.float32).reshape(ROWS, SEQ, KV, HQ_DEV + 2, HD)
    queries = projected[:, :, :, :HQ_DEV, :]
    key_part = projected[:, :, :, HQ_DEV, :]
    value_matrix = projected[:, :, :, HQ_DEV + 1, :].astype(bf)
    cosine_table, sine_table = rope_tables(positions, HD)
    rotary_queries = rotate(queries, cosine_table[:, :, None, None], sine_table[:, :, None, None]).astype(bf)
    rotary_keys = rotate(key_part, cosine_table[:, :, None], sine_table[:, :, None]).astype(bf)
    attention_output, log_total = lax.map(attend_row, (rotary_queries, rotary_keys, value_matrix, segments))
    attended_flat = attention_output.reshape(TOKENS, HEADS * HD)
    mixed_in = inputs + jnp.dot(attended_flat, w_out, preferred_element_type=jnp.float32)
    normed_two, inverse_two, hidden_two = rms_forward(mixed_in, gain_mlp)
    gate_vals = jnp.dot(hidden_two, w_gate, preferred_element_type=jnp.float32)
    up_vals = jnp.dot(hidden_two, w_up, preferred_element_type=jnp.float32)
    gate_sigmoid = jax.nn.sigmoid(gate_vals)
    activated = (gate_vals * gate_sigmoid * up_vals).astype(bf)
    result = mixed_in + jnp.dot(activated, w_down, preferred_element_type=jnp.float32)
    grad_b = grad_output.astype(bf)
    grad_w_down = tdot(activated, grad_b)
    grad_act = jnp.dot(grad_b, w_down.T, preferred_element_type=jnp.float32)
    grad_gate = (grad_act * up_vals * gate_sigmoid * (1.0 + gate_vals * (1.0 - gate_sigmoid))).astype(bf)
    grad_up = (grad_act * gate_vals * gate_sigmoid).astype(bf)
    grad_w_gate = tdot(hidden_two, grad_gate)
    grad_w_up = tdot(hidden_two, grad_up)
    grad_hidden_two = jnp.dot(grad_gate, w_gate.T, preferred_element_type=jnp.float32) + jnp.dot(grad_up, w_up.T, preferred_element_type=jnp.float32)
    grad_mixed, grad_gain_mlp = rms_backward(grad_output, grad_hidden_two, normed_two, inverse_two, gain_mlp)
    grad_mixed_b = grad_mixed.astype(bf)
    grad_w_out = tdot(attended_flat, grad_mixed_b)
    attention_output_gradient = jnp.dot(grad_mixed_b, w_out.T, preferred_element_type=jnp.float32).astype(bf).reshape(ROWS, SEQ, KV, HQ_DEV, HD)
    grad_qrot, grad_krot, grad_value = lax.map(attend_back_row, (rotary_queries, rotary_keys, value_matrix, segments, log_total, attention_output_gradient))
    grad_query = rotate(grad_qrot, cosine_table[:, :, None, None], -sine_table[:, :, None, None])
    grad_key = rotate(grad_krot, cosine_table[:, :, None], -sine_table[:, :, None])
    grad_qkv = jnp.concatenate([grad_query, grad_key[:, :, :, None, :], grad_value[:, :, :, None, :]], axis=3)
    grad_qkv = grad_qkv.reshape(TOKENS, KV * (HQ_DEV + 2) * HD).astype(bf)
    grad_w_qkv = tdot(hidden_one, grad_qkv)
    grad_hidden_one = jnp.dot(grad_qkv, w_qkv.T, preferred_element_type=jnp.float32)
    grad_inputs, grad_gain_attn = rms_backward(grad_mixed, grad_hidden_one, normed_one, inverse_one, gain_attn)
    return (result, grad_inputs, grad_gain_attn, grad_gain_mlp, grad_w_qkv, grad_w_out, grad_w_gate, grad_w_up, grad_w_down)
```

```python
import math

import jax
import jax.numpy as jnp
from jax import lax
from jax.sharding import PartitionSpec as P

D = 1536


EPS = 1e-05
ROPE_BASE = 100000.0
NEG_FILL = -1e30


def token_stats(values):
    return lax.psum(values, "row")


def widen(tensor):
    return lax.all_gather(tensor, "col", axis=0, tiled=True)


def narrow_sum(partial_sum):
    return lax.psum_scatter(partial_sum, "col", scatter_dimension=0, tiled=True)


def rows_sum(partial_sum):
    return lax.psum_scatter(partial_sum, "row", scatter_dimension=0, tiled=True)


def rows_gather(tensor):
    return lax.all_gather(tensor, "row", axis=0, tiled=True)


def norm_forward(values, gain_vec):
    totals = token_stats(jnp.sum(values * values, axis=1))
    inverse = lax.rsqrt(totals / D + EPS)[:, None]
    normed = values * inverse
    return (normed, inverse, (normed * gain_vec).astype(jnp.bfloat16))


def norm_backward(upstream, grad_hidden, normed, inverse, gain_vec):
    scaled = grad_hidden * gain_vec
    totals = token_stats(jnp.sum(scaled * normed, axis=1))
    centre = (totals / D)[:, None]
    return (upstream + inverse * (scaled - normed * centre), jnp.sum(grad_hidden * normed, axis=0))


def rope_tables(positions, head_size):
    half_size = head_size // 2
    frequency = ROPE_BASE ** (-(jnp.arange(half_size, dtype=jnp.float32) * 2.0 / head_size))
    angles = positions.astype(jnp.float32)[..., None] * frequency
    return (jnp.cos(angles), jnp.sin(angles))


def rotate(tensor, cosine_table, sine_table):
    half_size = tensor.shape[-1] // 2
    front_half = tensor[..., :half_size]
    back_half = tensor[..., half_size:]
    return jnp.concatenate(
        [
            front_half * cosine_table - back_half * sine_table,
            back_half * cosine_table + front_half * sine_table,
        ],
        axis=-1,
    )


def masked_scores(rotary_queries, rotary_keys, segments, score_scale):
    scores = (
        jnp.einsum(
            "nyrw,nzw->nryz", rotary_queries, rotary_keys, preferred_element_type=jnp.float32
        )
        * score_scale
    )
    order = jnp.arange(segments.shape[1])
    allowed = (segments[:, :, None] == segments[:, None, :]) & (order[:, None] >= order[None, :])[
        None
    ]
    return jnp.where(allowed[:, None], scores, NEG_FILL)


def attend_forward(rotary_queries, rotary_keys, value_matrix, segments, score_scale):
    scores = masked_scores(rotary_queries, rotary_keys, segments, score_scale)
    row_max = jnp.max(scores, axis=-1, keepdims=True)
    log_total = row_max + jnp.log(jnp.sum(jnp.exp(scores - row_max), axis=-1, keepdims=True))
    attention_weight_matrix = jnp.exp(scores - log_total).astype(jnp.bfloat16)
    attention_output = jnp.einsum(
        "uoap,upy->uaoy", attention_weight_matrix, value_matrix, preferred_element_type=jnp.float32
    )
    return (attention_output.astype(jnp.bfloat16), log_total)


def attend_backward(
    rotary_queries,
    rotary_keys,
    value_matrix,
    segments,
    log_total,
    attention_output_gradient,
    score_scale,
):
    scores = masked_scores(rotary_queries, rotary_keys, segments, score_scale)
    weights_f = jnp.exp(scores - log_total)
    grad_probs = jnp.einsum(
        "nyrw,nzw->nryz",
        attention_output_gradient,
        value_matrix,
        preferred_element_type=jnp.float32,
    )
    centre = jnp.sum(weights_f * grad_probs, axis=-1, keepdims=True)
    score_gradient = (weights_f * (grad_probs - centre)).astype(jnp.bfloat16)
    grad_qrot = (
        jnp.einsum(
            "uoap,upy->uaoy", score_gradient, rotary_keys, preferred_element_type=jnp.float32
        )
        * score_scale
    )
    grad_krot = (
        jnp.einsum(
            "ynep,yeno->ypo", score_gradient, rotary_queries, preferred_element_type=jnp.float32
        )
        * score_scale
    )
    grad_value = jnp.einsum(
        "ynep,yeno->ypo",
        weights_f.astype(jnp.bfloat16),
        attention_output_gradient,
        preferred_element_type=jnp.float32,
    )
    return (grad_qrot, grad_krot, grad_value)


def matmul(left, right):
    return jnp.dot(left, right, preferred_element_type=jnp.float32)


def left_t(left, right):
    return jnp.einsum("ta,tb->ab", left, right, preferred_element_type=jnp.float32)


def right_t(left, right):
    return jnp.einsum("tb,ab->ta", left, right, preferred_element_type=jnp.float32)


def shards(
    inputs,
    segments,
    positions,
    gain_attn,
    gain_mlp,
    w_qkv,
    w_out,
    w_gate,
    w_up,
    w_down,
    grad_output,
):
    bf = jnp.bfloat16
    seq_count, seq_len = segments.shape
    query_cols = w_out.shape[0]
    head_size = w_qkv.shape[1] - query_cols - (w_qkv.shape[1] - query_cols) // 2
    group_heads = query_cols // head_size
    local_tokens = seq_count * seq_len
    ff_cols = w_gate.shape[1]
    score_scale = 1.0 / math.sqrt(head_size)
    cosine_table, sine_table = rope_tables(positions, head_size)
    normed_one, inverse_one, hidden_one = norm_forward(inputs, gain_attn)
    wide_one = widen(hidden_one)
    qkv_local = rows_sum(matmul(wide_one, w_qkv))
    queries = qkv_local[:, :query_cols].reshape(seq_count, seq_len, group_heads, head_size)
    key_part = qkv_local[:, query_cols : query_cols + head_size].reshape(
        seq_count, seq_len, head_size
    )
    value_matrix = (
        qkv_local[:, query_cols + head_size :].reshape(seq_count, seq_len, head_size).astype(bf)
    )
    rotary_queries = rotate(queries, cosine_table[:, :, None, :], sine_table[:, :, None, :]).astype(
        bf
    )
    rotary_keys = rotate(key_part, cosine_table, sine_table).astype(bf)
    attention_output, log_total = attend_forward(
        rotary_queries, rotary_keys, value_matrix, segments, score_scale
    )
    attended_flat = attention_output.reshape(local_tokens, query_cols)
    wide_attended = rows_gather(attended_flat)
    mixed_in = inputs + narrow_sum(matmul(wide_attended, w_out))
    normed_two, inverse_two, hidden_two = norm_forward(mixed_in, gain_mlp)
    wide_two = widen(hidden_two)
    gate_up = rows_sum(jnp.concatenate([matmul(wide_two, w_gate), matmul(wide_two, w_up)], axis=1))
    gate_vals = gate_up[:, :ff_cols]
    up_vals = gate_up[:, ff_cols:]
    gate_sigmoid = jax.nn.sigmoid(gate_vals)
    activated = (gate_vals * gate_sigmoid * up_vals).astype(bf)
    wide_act = rows_gather(activated)
    result = mixed_in + narrow_sum(matmul(wide_act, w_down))
    grad_wide = widen(grad_output.astype(bf))
    grad_w_down = left_t(wide_act, grad_wide)
    grad_act = rows_sum(right_t(grad_wide, w_down))
    grad_gate = (
        grad_act * up_vals * gate_sigmoid * (1.0 + gate_vals * (1.0 - gate_sigmoid))
    ).astype(bf)
    grad_up = (grad_act * gate_vals * gate_sigmoid).astype(bf)
    wide_grads = rows_gather(jnp.concatenate([grad_gate, grad_up], axis=1))
    grad_w_gate = left_t(wide_two, wide_grads[:, :ff_cols])
    grad_w_up = left_t(wide_two, wide_grads[:, ff_cols:])
    grad_hidden_two = narrow_sum(
        right_t(wide_grads[:, :ff_cols], w_gate) + right_t(wide_grads[:, ff_cols:], w_up)
    )
    grad_mixed, grad_gain_mlp = norm_backward(
        grad_output, grad_hidden_two, normed_two, inverse_two, gain_mlp
    )
    grad_mixed_wide = widen(grad_mixed.astype(bf))
    grad_w_out = left_t(wide_attended, grad_mixed_wide)
    attention_output_gradient = (
        rows_sum(right_t(grad_mixed_wide, w_out))
        .astype(bf)
        .reshape(seq_count, seq_len, group_heads, head_size)
    )
    grad_qrot, grad_krot, grad_value = attend_backward(
        rotary_queries,
        rotary_keys,
        value_matrix,
        segments,
        log_total,
        attention_output_gradient,
        score_scale,
    )
    grad_query = rotate(grad_qrot, cosine_table[:, :, None, :], -sine_table[:, :, None, :]).reshape(
        local_tokens, query_cols
    )
    grad_key = rotate(grad_krot, cosine_table, -sine_table).reshape(local_tokens, head_size)
    grad_qkv = jnp.concatenate(
        [grad_query, grad_key, grad_value.reshape(local_tokens, head_size)], axis=1
    ).astype(bf)
    wide_qkv = rows_gather(grad_qkv)
    grad_w_qkv = left_t(wide_one, wide_qkv)
    grad_hidden_one = narrow_sum(right_t(wide_qkv, w_qkv))
    grad_inputs, grad_gain_attn = norm_backward(
        grad_mixed, grad_hidden_one, normed_one, inverse_one, gain_attn
    )
    grad_gain_attn, grad_gain_mlp = lax.psum((grad_gain_attn, grad_gain_mlp), ("batch", "col"))
    grad_w_qkv, grad_w_out, grad_w_gate, grad_w_up, grad_w_down = (
        lax.psum(grad_w_qkv.astype(jnp.bfloat16), "batch").astype(jnp.float32),
        lax.psum(grad_w_out.astype(jnp.bfloat16), "batch").astype(jnp.float32),
        lax.psum(grad_w_gate.astype(jnp.bfloat16), "batch").astype(jnp.float32),
        lax.psum(grad_w_up.astype(jnp.bfloat16), "batch").astype(jnp.float32),
        lax.psum(grad_w_down.astype(jnp.bfloat16), "batch").astype(jnp.float32),
    )
    return (
        result,
        grad_inputs,
        grad_gain_attn,
        grad_gain_mlp,
        grad_w_qkv,
        grad_w_out,
        grad_w_gate,
        grad_w_up,
        grad_w_down,
    )


def swap_row(tensor):
    return lax.ppermute(tensor, "row", [(0, 1), (1, 0)])


def swap_core(tensor):
    return lax.ppermute(tensor, "batch", [(0, 1), (1, 0), (2, 3), (3, 2)])


def swap_chip(tensor):
    return lax.ppermute(tensor, "batch", [(0, 2), (2, 0), (1, 3), (3, 1)])


def pick(tensor, index, axis=0):
    return lax.dynamic_index_in_dim(tensor, index, axis, keepdims=False)


def in_order(mine, other, index, axis=0):
    first = jnp.where(index == 0, mine, other)
    second = jnp.where(index == 0, other, mine)
    return jnp.stack([first, second], axis=axis)


def gather_team(tensor):
    full = lax.all_gather(tensor, ("batch", "row"), axis=0, tiled=False)
    full = full.reshape(4, 2, *tensor.shape)
    return jnp.transpose(full, (0, 2, 1, 3))


def scatter_team(partial):
    parts = jnp.transpose(partial, (0, 2, 1, 3)).reshape(8, partial.shape[1], partial.shape[3])
    return lax.psum_scatter(parts, ("batch", "row"), scatter_dimension=0, tiled=False)


def fast_shards(
    inputs,
    segments,
    positions,
    gain_attn,
    gain_mlp,
    w_qkv,
    w_out,
    w_gate,
    w_up,
    w_down,
    grad_output,
):
    bf = jnp.bfloat16
    f32 = jnp.float32
    b = lax.axis_index("batch")
    y = lax.axis_index("row")
    z = lax.axis_index("col")
    c = lax.rem(b, 2)
    cols = lax.axis_size("col")
    seq_len = segments.shape[1]
    tokens, feats = inputs.shape
    query_cols = w_out.shape[0]
    block_cols = w_qkv.shape[1]
    head_size = block_cols - query_cols - (block_cols - query_cols) // 2
    group_heads = query_cols // head_size
    score_scale = 1.0 / math.sqrt(head_size)
    ff_cols = w_gate.shape[1]
    part = ff_cols // 8

    def eighth(index):
        return jnp.stack(
            [
                lax.dynamic_slice_in_dim(w_gate, index * part, part, 1).T,
                lax.dynamic_slice_in_dim(w_up, index * part, part, 1).T,
                lax.dynamic_slice_in_dim(w_down, index * part, part, 0),
            ]
        )

    mine_w = eighth(2 * b + y)
    their_w = swap_row(eighth(2 * b + 1 - y))
    full_w = jnp.concatenate(
        [jnp.where(y == 0, mine_w, their_w), jnp.where(y == 0, their_w, mine_w)], axis=2
    )
    gate_up_w = lax.all_gather(full_w[:2], "col", axis=1, tiled=True)
    down_w = lax.all_gather(full_w[2], "col", axis=0, tiled=True)
    gate_w, up_w = gate_up_w[0], gate_up_w[1]

    places = jnp.stack([segments, positions])
    places = in_order(places, swap_row(places), y, axis=1).reshape(2, 4, seq_len)
    places = pick(places, z, 1)
    places = in_order(places, swap_core(places), c, axis=1)
    seg, pos = places[0], places[1]
    cosine_table, sine_table = rope_tables(pos, head_size)

    wa = jnp.concatenate([w_qkv, w_out.T], axis=1)
    wa = lax.all_gather(wa, "col", axis=0, tiled=False)
    wa = lax.dynamic_slice_in_dim(wa, 2 * c, 2, 0)
    wa_mine, wa_theirs = pick(wa, y), pick(wa, 1 - y)
    wq_mine, wo_mine = wa_mine[:, :block_cols], wa_mine[:, block_cols:]
    wq_theirs, wo_theirs = wa_theirs[:, :block_cols], wa_theirs[:, block_cols:]

    normed_one, inverse_one, hidden_one = norm_forward(inputs, gain_attn)
    wide_one = in_order(hidden_one, swap_core(hidden_one), c).reshape(2 * tokens, feats)
    sent = matmul(wide_one, wq_theirs).astype(bf)
    qkv_local = matmul(wide_one, wq_mine) + swap_row(sent).astype(f32)
    seq_count = 2
    queries = qkv_local[:, :query_cols].reshape(seq_count, seq_len, group_heads, head_size)
    key_part = qkv_local[:, query_cols : query_cols + head_size].reshape(
        seq_count, seq_len, head_size
    )
    value_matrix = (
        qkv_local[:, query_cols + head_size :].reshape(seq_count, seq_len, head_size).astype(bf)
    )
    rotary_queries = rotate(queries, cosine_table[:, :, None, :], sine_table[:, :, None, :]).astype(
        bf
    )
    rotary_keys = rotate(key_part, cosine_table, sine_table).astype(bf)
    attention_output, log_total = attend_forward(
        rotary_queries, rotary_keys, value_matrix, seg, score_scale
    )
    attended = attention_output.reshape(2 * tokens, query_cols)
    attended_theirs = swap_row(attended)
    out_partial = right_t(attended, wo_mine) + right_t(attended_theirs, wo_theirs)
    out_partial = out_partial.reshape(2, tokens, feats)
    mixed_in = inputs + (pick(out_partial, c) + swap_core(pick(out_partial, 1 - c)))
    normed_two, inverse_two, hidden_two = norm_forward(mixed_in, gain_mlp)

    wide_two = gather_team(hidden_two).reshape(4 * tokens, 2 * feats)
    gate_vals = right_t(wide_two, gate_w)
    up_vals = right_t(wide_two, up_w)
    gate_sigmoid = jax.nn.sigmoid(gate_vals)
    activated = (gate_vals * gate_sigmoid * up_vals).astype(bf)
    result_partial = matmul(activated, down_w).astype(bf).reshape(4, tokens, 2, feats)
    result = mixed_in + scatter_team(result_partial).astype(f32)

    wide_grad = gather_team(grad_output.astype(bf)).reshape(4 * tokens, 2 * feats)
    grad_act = right_t(wide_grad, down_w)
    grad_w_down = left_t(activated, wide_grad).astype(bf)
    grad_gate = (
        grad_act * up_vals * gate_sigmoid * (1.0 + gate_vals * (1.0 - gate_sigmoid))
    ).astype(bf)
    grad_up = (grad_act * gate_vals * gate_sigmoid).astype(bf)
    grad_w_gate = left_t(grad_gate, wide_two).astype(bf)
    grad_w_up = left_t(grad_up, wide_two).astype(bf)
    hidden_partial = matmul(grad_gate, gate_w) + matmul(grad_up, up_w)
    grad_hidden_two = scatter_team(hidden_partial.astype(bf).reshape(4, tokens, 2, feats)).astype(
        f32
    )
    grad_mixed, grad_gain_mlp = norm_backward(
        grad_output, grad_hidden_two, normed_two, inverse_two, gain_mlp
    )

    grad_mixed_b = grad_mixed.astype(bf)
    wide_mixed = in_order(grad_mixed_b, swap_core(grad_mixed_b), c).reshape(2 * tokens, feats)
    grad_wo_mine = left_t(wide_mixed, attended)
    grad_wo_theirs = left_t(wide_mixed, attended_theirs)
    sent = matmul(wide_mixed, wo_theirs).astype(bf)
    attention_output_gradient = (
        (matmul(wide_mixed, wo_mine) + swap_row(sent).astype(f32))
        .astype(bf)
        .reshape(seq_count, seq_len, group_heads, head_size)
    )
    grad_qrot, grad_krot, grad_value = attend_backward(
        rotary_queries,
        rotary_keys,
        value_matrix,
        seg,
        log_total,
        attention_output_gradient,
        score_scale,
    )
    grad_query = rotate(grad_qrot, cosine_table[:, :, None, :], -sine_table[:, :, None, :]).reshape(
        2 * tokens, query_cols
    )
    grad_key = rotate(grad_krot, cosine_table, -sine_table).reshape(2 * tokens, head_size)
    grad_qkv = jnp.concatenate(
        [grad_query, grad_key, grad_value.reshape(2 * tokens, head_size)], axis=1
    ).astype(bf)
    grad_qkv_theirs = swap_row(grad_qkv)
    one_partial = right_t(grad_qkv, wq_mine) + right_t(grad_qkv_theirs, wq_theirs)
    one_partial = one_partial.reshape(2, tokens, feats)
    grad_hidden_one = pick(one_partial, c) + swap_core(pick(one_partial, 1 - c))
    grad_inputs, grad_gain_attn = norm_backward(
        grad_mixed, grad_hidden_one, normed_one, inverse_one, gain_attn
    )
    grad_gain_attn, grad_gain_mlp = lax.psum((grad_gain_attn, grad_gain_mlp), ("batch", "col"))

    grad_wq = in_order(left_t(wide_one, grad_qkv), left_t(wide_one, grad_qkv_theirs), y)
    grad_wo = in_order(grad_wo_mine, grad_wo_theirs, y)
    grad_wa = jnp.concatenate([grad_wq, grad_wo], axis=2).astype(bf)
    blank = jnp.zeros_like(grad_wa)
    grad_wa = jnp.concatenate(
        [jnp.where(c == 0, grad_wa, blank), jnp.where(c == 0, blank, grad_wa)], axis=0
    )
    grad_wa = lax.psum_scatter(grad_wa, "col", scatter_dimension=0, tiled=False)
    grad_wa = lax.psum(grad_wa, "batch").astype(f32)
    grad_w_qkv = grad_wa[:, :block_cols]
    grad_w_out = grad_wa[:, block_cols:].T

    def assemble(stacked):
        summed = lax.psum_scatter(stacked, "col", scatter_dimension=1, tiled=True)
        halves = summed.reshape(-1, part, 2, feats)
        mine, theirs = pick(halves, y, 2), pick(halves, 1 - y, 2)
        pair = in_order(mine, swap_row(theirs), y, axis=1)
        return lax.all_gather(pair, "batch", axis=1, tiled=False).reshape(-1, ff_cols, feats)

    grad_w_down = assemble(grad_w_down[None])[0].astype(f32)
    grads = assemble(jnp.stack([grad_w_gate, grad_w_up]))
    grad_w_gate = grads[0].T.astype(f32)
    grad_w_up = grads[1].T.astype(f32)
    return (
        result,
        grad_inputs,
        grad_gain_attn,
        grad_gain_mlp,
        grad_w_qkv,
        grad_w_out,
        grad_w_gate,
        grad_w_up,
        grad_w_down,
    )


def solution(mesh):
    shape = mesh.shape
    team = shape["batch"] == 4 and shape["row"] == 2 and shape["col"] == 4
    return jax.shard_map(
        fast_shards if team else shards,
        mesh=mesh,
        in_specs=(
            P(("batch", "col"), "row"),
            P(("batch", "row"), None),
            P(("batch", "row"), None),
            P("row"),
            P("row"),
            P("row", "col"),
            P("col", "row"),
            P("row", "col"),
            P("row", "col"),
            P("col", "row"),
            P(("batch", "col"), "row"),
        ),
        out_specs=(
            P(("batch", "col"), "row"),
            P(("batch", "col"), "row"),
            P("row"),
            P("row"),
            P("row", "col"),
            P("col", "row"),
            P("row", "col"),
            P("row", "col"),
            P("col", "row"),
        ),
        check_vma=False,
    )
```

```python
import functools
import math

import jax
import jax.numpy as jnp
from jax import lax
from jax.experimental import pallas as pl
from jax.experimental.pallas import tpu as pltpu
from jax.sharding import PartitionSpec as P

D = 1536


EPS = 1e-05
ROPE_BASE = 100000.0
NEG_FILL = -1e30


def token_stats(values):
    return lax.psum(values, "row")


def widen(tensor):
    return lax.all_gather(tensor, "col", axis=0, tiled=True)


def narrow_sum(partial_sum):
    return lax.psum_scatter(partial_sum, "col", scatter_dimension=0, tiled=True)


def rows_sum(partial_sum):
    return lax.psum_scatter(partial_sum, "row", scatter_dimension=0, tiled=True)


def rows_gather(tensor):
    return lax.all_gather(tensor, "row", axis=0, tiled=True)


def norm_forward(values, gain_vec):
    totals = token_stats(jnp.sum(values * values, axis=1))
    inverse = lax.rsqrt(totals / D + EPS)[:, None]
    normed = values * inverse
    return (normed, inverse, (normed * gain_vec).astype(jnp.bfloat16))


def norm_backward(upstream, grad_hidden, normed, inverse, gain_vec):
    scaled = grad_hidden * gain_vec
    totals = token_stats(jnp.sum(scaled * normed, axis=1))
    centre = (totals / D)[:, None]
    return (upstream + inverse * (scaled - normed * centre), jnp.sum(grad_hidden * normed, axis=0))


def rope_tables(positions, head_size):
    half_size = head_size // 2
    frequency = ROPE_BASE ** (-(jnp.arange(half_size, dtype=jnp.float32) * 2.0 / head_size))
    angles = positions.astype(jnp.float32)[..., None] * frequency
    return (jnp.cos(angles), jnp.sin(angles))


def rotate(tensor, cosine_table, sine_table):
    half_size = tensor.shape[-1] // 2
    front_half = tensor[..., :half_size]
    back_half = tensor[..., half_size:]
    return jnp.concatenate(
        [
            front_half * cosine_table - back_half * sine_table,
            back_half * cosine_table + front_half * sine_table,
        ],
        axis=-1,
    )


def masked_scores(rotary_queries, rotary_keys, segments, score_scale):
    scores = (
        jnp.einsum(
            "nyrw,nzw->nryz", rotary_queries, rotary_keys, preferred_element_type=jnp.float32
        )
        * score_scale
    )
    order = jnp.arange(segments.shape[1])
    allowed = (segments[:, :, None] == segments[:, None, :]) & (order[:, None] >= order[None, :])[
        None
    ]
    return jnp.where(allowed[:, None], scores, NEG_FILL)


def attend_forward(rotary_queries, rotary_keys, value_matrix, segments, score_scale):
    scores = masked_scores(rotary_queries, rotary_keys, segments, score_scale)
    row_max = jnp.max(scores, axis=-1, keepdims=True)
    log_total = row_max + jnp.log(jnp.sum(jnp.exp(scores - row_max), axis=-1, keepdims=True))
    attention_weight_matrix = jnp.exp(scores - log_total).astype(jnp.bfloat16)
    attention_output = jnp.einsum(
        "uoap,upy->uaoy", attention_weight_matrix, value_matrix, preferred_element_type=jnp.float32
    )
    return (attention_output.astype(jnp.bfloat16), log_total)


def attend_backward(
    rotary_queries,
    rotary_keys,
    value_matrix,
    segments,
    log_total,
    attention_output_gradient,
    score_scale,
):
    scores = masked_scores(rotary_queries, rotary_keys, segments, score_scale)
    weights_f = jnp.exp(scores - log_total)
    grad_probs = jnp.einsum(
        "nyrw,nzw->nryz",
        attention_output_gradient,
        value_matrix,
        preferred_element_type=jnp.float32,
    )
    centre = jnp.sum(weights_f * grad_probs, axis=-1, keepdims=True)
    score_gradient = (weights_f * (grad_probs - centre)).astype(jnp.bfloat16)
    grad_qrot = (
        jnp.einsum(
            "uoap,upy->uaoy", score_gradient, rotary_keys, preferred_element_type=jnp.float32
        )
        * score_scale
    )
    grad_krot = (
        jnp.einsum(
            "ynep,yeno->ypo", score_gradient, rotary_queries, preferred_element_type=jnp.float32
        )
        * score_scale
    )
    grad_value = jnp.einsum(
        "ynep,yeno->ypo",
        weights_f.astype(jnp.bfloat16),
        attention_output_gradient,
        preferred_element_type=jnp.float32,
    )
    return (grad_qrot, grad_krot, grad_value)


def matmul(left, right):
    return jnp.dot(left, right, preferred_element_type=jnp.float32)


def left_t(left, right):
    return jnp.einsum("ta,tb->ab", left, right, preferred_element_type=jnp.float32)


def right_t(left, right):
    return jnp.einsum("tb,ab->ta", left, right, preferred_element_type=jnp.float32)


def shards(
    inputs,
    segments,
    positions,
    gain_attn,
    gain_mlp,
    w_qkv,
    w_out,
    w_gate,
    w_up,
    w_down,
    grad_output,
):
    bf = jnp.bfloat16
    seq_count, seq_len = segments.shape
    query_cols = w_out.shape[0]
    head_size = w_qkv.shape[1] - query_cols - (w_qkv.shape[1] - query_cols) // 2
    group_heads = query_cols // head_size
    local_tokens = seq_count * seq_len
    ff_cols = w_gate.shape[1]
    score_scale = 1.0 / math.sqrt(head_size)
    cosine_table, sine_table = rope_tables(positions, head_size)
    normed_one, inverse_one, hidden_one = norm_forward(inputs, gain_attn)
    wide_one = widen(hidden_one)
    qkv_local = rows_sum(matmul(wide_one, w_qkv))
    queries = qkv_local[:, :query_cols].reshape(seq_count, seq_len, group_heads, head_size)
    key_part = qkv_local[:, query_cols : query_cols + head_size].reshape(
        seq_count, seq_len, head_size
    )
    value_matrix = (
        qkv_local[:, query_cols + head_size :].reshape(seq_count, seq_len, head_size).astype(bf)
    )
    rotary_queries = rotate(queries, cosine_table[:, :, None, :], sine_table[:, :, None, :]).astype(
        bf
    )
    rotary_keys = rotate(key_part, cosine_table, sine_table).astype(bf)
    attention_output, log_total = attend_forward(
        rotary_queries, rotary_keys, value_matrix, segments, score_scale
    )
    attended_flat = attention_output.reshape(local_tokens, query_cols)
    wide_attended = rows_gather(attended_flat)
    mixed_in = inputs + narrow_sum(matmul(wide_attended, w_out))
    normed_two, inverse_two, hidden_two = norm_forward(mixed_in, gain_mlp)
    wide_two = widen(hidden_two)
    gate_up = rows_sum(jnp.concatenate([matmul(wide_two, w_gate), matmul(wide_two, w_up)], axis=1))
    gate_vals = gate_up[:, :ff_cols]
    up_vals = gate_up[:, ff_cols:]
    gate_sigmoid = jax.nn.sigmoid(gate_vals)
    activated = (gate_vals * gate_sigmoid * up_vals).astype(bf)
    wide_act = rows_gather(activated)
    result = mixed_in + narrow_sum(matmul(wide_act, w_down))
    grad_wide = widen(grad_output.astype(bf))
    grad_w_down = left_t(wide_act, grad_wide)
    grad_act = rows_sum(right_t(grad_wide, w_down))
    grad_gate = (
        grad_act * up_vals * gate_sigmoid * (1.0 + gate_vals * (1.0 - gate_sigmoid))
    ).astype(bf)
    grad_up = (grad_act * gate_vals * gate_sigmoid).astype(bf)
    wide_grads = rows_gather(jnp.concatenate([grad_gate, grad_up], axis=1))
    grad_w_gate = left_t(wide_two, wide_grads[:, :ff_cols])
    grad_w_up = left_t(wide_two, wide_grads[:, ff_cols:])
    grad_hidden_two = narrow_sum(
        right_t(wide_grads[:, :ff_cols], w_gate) + right_t(wide_grads[:, ff_cols:], w_up)
    )
    grad_mixed, grad_gain_mlp = norm_backward(
        grad_output, grad_hidden_two, normed_two, inverse_two, gain_mlp
    )
    grad_mixed_wide = widen(grad_mixed.astype(bf))
    grad_w_out = left_t(wide_attended, grad_mixed_wide)
    attention_output_gradient = (
        rows_sum(right_t(grad_mixed_wide, w_out))
        .astype(bf)
        .reshape(seq_count, seq_len, group_heads, head_size)
    )
    grad_qrot, grad_krot, grad_value = attend_backward(
        rotary_queries,
        rotary_keys,
        value_matrix,
        segments,
        log_total,
        attention_output_gradient,
        score_scale,
    )
    grad_query = rotate(grad_qrot, cosine_table[:, :, None, :], -sine_table[:, :, None, :]).reshape(
        local_tokens, query_cols
    )
    grad_key = rotate(grad_krot, cosine_table, -sine_table).reshape(local_tokens, head_size)
    grad_qkv = jnp.concatenate(
        [grad_query, grad_key, grad_value.reshape(local_tokens, head_size)], axis=1
    ).astype(bf)
    wide_qkv = rows_gather(grad_qkv)
    grad_w_qkv = left_t(wide_one, wide_qkv)
    grad_hidden_one = narrow_sum(right_t(wide_qkv, w_qkv))
    grad_inputs, grad_gain_attn = norm_backward(
        grad_mixed, grad_hidden_one, normed_one, inverse_one, gain_attn
    )
    grad_gain_attn, grad_gain_mlp = lax.psum((grad_gain_attn, grad_gain_mlp), ("batch", "col"))
    grad_w_qkv, grad_w_out, grad_w_gate, grad_w_up, grad_w_down = (
        lax.psum(grad_w_qkv.astype(jnp.bfloat16), "batch").astype(jnp.float32),
        lax.psum(grad_w_out.astype(jnp.bfloat16), "batch").astype(jnp.float32),
        lax.psum(grad_w_gate.astype(jnp.bfloat16), "batch").astype(jnp.float32),
        lax.psum(grad_w_up.astype(jnp.bfloat16), "batch").astype(jnp.float32),
        lax.psum(grad_w_down.astype(jnp.bfloat16), "batch").astype(jnp.float32),
    )
    return (
        result,
        grad_inputs,
        grad_gain_attn,
        grad_gain_mlp,
        grad_w_qkv,
        grad_w_out,
        grad_w_gate,
        grad_w_up,
        grad_w_down,
    )


MESH = pl.DeviceIdType.MESH


def place(b, y, z):
    return {"batch": b, "row": y, "col": z}


def me():
    return lax.axis_index("batch"), lax.axis_index("row"), lax.axis_index("col")


def greet(partners):
    barrier = pltpu.get_barrier_semaphore()
    for partner in partners:
        pl.semaphore_signal(barrier, inc=1, device_id=partner, device_id_type=MESH)
    pl.semaphore_wait(barrier, len(partners))


def send(src, dst, send_sem, recv_sem, target):
    copy = pltpu.make_async_remote_copy(
        src_ref=src,
        dst_ref=dst,
        send_sem=send_sem,
        recv_sem=recv_sem,
        device_id=target,
        device_id_type=MESH,
    )
    copy.start()
    return copy


def landed(ref, sem):
    pltpu.make_async_copy(ref, ref, sem).wait()


def xor(index, bit):
    return index + bit - 2 * bit * lax.rem(lax.div(index, jnp.int32(bit)), 2)


def dot_t(left, right):
    return lax.dot_general(left, right, (((1,), (1,)), ((), ())), preferred_element_type=jnp.float32)


OWN, SIB, FAR, FAR_SIB = range(4)


def gate_up_kernel(
    hid, wg, wu, wide, gate, up, act, wide_v, wg_v, wu_v, gate_v, up_v, act_v,
    own_send, fwd_send, recv, local, out_sem,
):
    b, y, z = me()
    tokens, feats = hid.shape
    half = tokens // 2
    near, across, beside = place(xor(b, 1), y, z), place(xor(b, 2), y, z), place(b, 1 - y, z)
    loads = [
        pltpu.make_async_copy(hid, wide_v.at[0, OWN], local.at[0]),
        pltpu.make_async_copy(wg, wg_v, local.at[1]),
        pltpu.make_async_copy(wu, wu_v, local.at[2]),
    ]
    for load in loads:
        load.start()
    greet([near, across, beside])

    def rows(h):
        return pl.ds(h * half, half)

    copies = []
    for i in (0, 1):
        for t, (target, yy, bb, h) in enumerate(
            ((across, 0, FAR, i), (beside, 1, OWN, 1 - i), (near, 0, SIB, i))
        ):
            copies.append(
                send(
                    hid.at[rows(h)], wide_v.at[yy, bb, rows(h)], own_send.at[t, i], recv.at[yy, bb, h], target
                )
            )
    for load in loads:
        load.wait()

    def forward(slot, yy, bb, h, target, to_y, to_b):
        copies.append(
            send(
                wide_v.at[yy, bb, rows(h)],
                wide_v.at[to_y, to_b, rows(h)],
                fwd_send.at[slot],
                recv.at[to_y, to_b, h],
                target,
            )
        )

    def arrive(yy, bb, h):
        landed(wide_v.at[yy, bb, rows(h)], recv.at[yy, bb, h])

    step = 256

    def work(yy, bb, h, first):
        for w_v, total in ((wg_v, gate_v), (wu_v, up_v)):

            def body(i, _, w_v=w_v, total=total):
                out = pl.ds(pl.multiple_of(i * step, step), step)
                value = dot_t(wide_v[yy, bb, rows(h), :], w_v[out, pl.ds(yy * feats, feats)])
                if first:
                    total[bb, rows(h), out] = value
                else:
                    total[bb, rows(h), out] += value
                return 0

            lax.fori_loop(0, w_v.shape[0] // step, body, 0)

    def finish(bb, h):
        chunk = 32

        def body(i, _):
            r = pl.ds(pl.multiple_of(h * half + i * chunk, chunk), chunk)
            g = gate_v[bb, r, :]
            act_v[bb, r, :] = (g * jax.nn.sigmoid(g) * up_v[bb, r, :]).astype(act_v.dtype)
            return 0

        lax.fori_loop(0, half // chunk, body, 0)
        for k, (src, dst) in enumerate(((gate_v, gate), (up_v, up), (act_v, act))):
            pltpu.make_async_copy(src.at[bb, rows(h)], dst.at[bb, rows(h)], out_sem.at[k]).start()

    work(0, OWN, 0, True)
    work(0, OWN, 1, True)
    arrive(0, SIB, 0)
    work(0, SIB, 0, True)
    arrive(0, SIB, 1)
    work(0, SIB, 1, True)
    arrive(0, FAR, 0)
    forward(0, 0, FAR, 0, near, 0, FAR_SIB)
    forward(1, 0, FAR, 0, beside, 1, FAR)
    arrive(1, OWN, 1)
    forward(2, 1, OWN, 1, near, 1, SIB)
    forward(3, 1, OWN, 1, across, 1, FAR)
    work(0, FAR, 0, True)
    work(1, OWN, 1, False)
    finish(OWN, 1)
    arrive(0, FAR_SIB, 0)
    work(0, FAR_SIB, 0, True)
    arrive(1, SIB, 1)
    work(1, SIB, 1, False)
    finish(SIB, 1)
    arrive(0, FAR, 1)
    forward(4, 0, FAR, 1, near, 0, FAR_SIB)
    arrive(1, OWN, 0)
    forward(5, 1, OWN, 0, near, 1, SIB)
    work(0, FAR, 1, True)
    work(1, OWN, 0, False)
    finish(OWN, 0)
    arrive(0, FAR_SIB, 1)
    work(0, FAR_SIB, 1, True)
    arrive(1, SIB, 0)
    work(1, SIB, 0, False)
    finish(SIB, 0)
    arrive(1, FAR, 0)
    forward(6, 1, FAR, 0, near, 1, FAR_SIB)
    arrive(1, FAR, 1)
    forward(7, 1, FAR, 1, near, 1, FAR_SIB)
    work(1, FAR, 0, False)
    finish(FAR, 0)
    work(1, FAR, 1, False)
    finish(FAR, 1)
    arrive(1, FAR_SIB, 0)
    arrive(1, FAR_SIB, 1)
    saves = [
        pltpu.make_async_copy(wide_v.at[yy], wide.at[:, :, pl.ds(yy * feats, feats)], local.at[yy])
        for yy in (0, 1)
    ]
    for save in saves:
        save.start()
    work(1, FAR_SIB, 0, False)
    finish(FAR_SIB, 0)
    work(1, FAR_SIB, 1, False)
    finish(FAR_SIB, 1)
    for copy in copies:
        copy.wait_send()
    for save in saves:
        save.wait()
    for k, (src, dst) in enumerate(((gate_v, gate), (up_v, up), (act_v, act))):
        pltpu.make_async_copy(src, dst, out_sem.at[k]).wait()


def gate_up(hidden, gate_w, up_w):
    tokens, feats = hidden.shape
    width = gate_w.shape[0]
    bf, f32 = jnp.bfloat16, jnp.float32
    any_spec = pl.BlockSpec(memory_space=pl.ANY)
    dma = pltpu.SemaphoreType.DMA
    return pl.pallas_call(
        gate_up_kernel,
        out_shape=(
            jax.ShapeDtypeStruct((4, tokens, 2 * feats), bf),
            jax.ShapeDtypeStruct((4, tokens, width), f32),
            jax.ShapeDtypeStruct((4, tokens, width), f32),
            jax.ShapeDtypeStruct((4, tokens, width), bf),
        ),
        in_specs=[any_spec] * 3,
        out_specs=(any_spec,) * 4,
        scratch_shapes=[
            pltpu.VMEM((2, 4, tokens, feats), bf),
            pltpu.VMEM((width, 2 * feats), bf),
            pltpu.VMEM((width, 2 * feats), bf),
            pltpu.VMEM((4, tokens, width), f32),
            pltpu.VMEM((4, tokens, width), f32),
            pltpu.VMEM((4, tokens, width), bf),
            dma((3, 2)),
            dma((8,)),
            dma((2, 4, 2)),
            dma((3,)),
            dma((3,)),
        ],
        compiler_params=pltpu.CompilerParams(
            collective_id=1, has_side_effects=True, vmem_limit_bytes=48 * 2**20
        ),
        cost_estimate=pl.CostEstimate(
            flops=2 * 8 * tokens * feats * 2 * width, bytes_accessed=30 * 2**20, transcendentals=0
        ),
        name="gate_up",
    )(hidden, gate_w, up_w)


def team_sum_kernel(pairs, *refs):
    lefts, rights = refs[:pairs], refs[pairs : 2 * pairs]
    out = refs[2 * pairs]
    scratch = refs[2 * pairs + 1 :]
    lefts_v, rights_v = scratch[:pairs], scratch[pairs : 2 * pairs]
    (
        own, near_out, near_in, turn, turn_x, turn_y, far_out, far_in, side_out, side_in,
        load_sem, near_send, near_recv, turn_send, turn_recv, link_send, link_recv, out_sem,
    ) = scratch[2 * pairs :]
    b, y, z = me()
    tokens, feats = out.shape
    half = tokens // 2
    near, across, beside = place(xor(b, 1), y, z), place(xor(b, 2), y, z), place(b, 1 - y, z)
    loads = []
    for i in range(pairs):
        loads.append(pltpu.make_async_copy(rights[i], rights_v[i], load_sem.at[i, 0]))
        loads.append(pltpu.make_async_copy(lefts[i], lefts_v[i], load_sem.at[i, 1]))
    for load in loads:
        load.start()
    greet([near, across, beside])
    for load in loads:
        load.wait()

    def rows(h):
        return pl.ds(h * half, half)

    step = 256

    def product(bb, yy, store):
        def body(i, _):
            r = pl.ds(pl.multiple_of((i // 3) * step, step), step)
            n = lax.rem(i, 3) * step
            cols = pl.ds(pl.multiple_of(yy * feats + n, 128), step)
            value = jnp.dot(lefts_v[0][bb, r, :], rights_v[0][:, cols], preferred_element_type=jnp.float32)
            for j in range(1, pairs):
                value += jnp.dot(lefts_v[j][bb, r, :], rights_v[j][:, cols], preferred_element_type=jnp.float32)
            store(r, pl.ds(pl.multiple_of(n, 128), step), value)
            return 0

        lax.fori_loop(0, (tokens // step) * (feats // step), body, 0)

    copies = []
    order = ((FAR, FAR_SIB, 1), (FAR, FAR_SIB, 0), (OWN, SIB, 1), (OWN, SIB, 0))
    for k, (mine, theirs, yy) in enumerate(order):

        def keep_near(r, cols, value, k=k):
            near_out[k, r, cols] = value.astype(near_out.dtype)

        def keep_own(r, cols, value, k=k):
            own[k, r, cols] = value

        product(theirs, yy, keep_near)
        copies.append(send(near_out.at[k], near_in.at[k], near_send.at[k], near_recv.at[k], near))
        product(mine, yy, keep_own)
        if k == 0:
            landed(near_in.at[0], near_recv.at[0])
            add_rows(turn, own, near_in, 0, 0, tokens)
            copies.append(send(turn.at[rows(0)], turn_x, turn_send.at[0], turn_recv.at[0], across))
            copies.append(send(turn.at[rows(1)], turn_y, turn_send.at[1], turn_recv.at[1], beside))
        if k == 1:
            landed(near_in.at[1], near_recv.at[1])
            add_rows(far_out, own, near_in, 1, 0, half)
            copies.append(send(far_out.at[rows(0)], far_in.at[rows(0)], link_send.at[0], link_recv.at[0], across))
        if k == 2:
            landed(near_in.at[2], near_recv.at[2])
            add_rows(side_out, own, near_in, 2, half, half)
            copies.append(send(side_out.at[rows(1)], side_in.at[rows(1)], link_send.at[1], link_recv.at[1], beside))
    landed(turn_y, turn_recv.at[1])
    add_rows(far_out, own, near_in, 1, half, half, turn_y, half)
    copies.append(send(far_out.at[rows(1)], far_in.at[rows(1)], link_send.at[2], link_recv.at[2], across))
    landed(turn_x, turn_recv.at[0])
    add_rows(side_out, own, near_in, 2, 0, half, turn_x, 0)
    copies.append(send(side_out.at[rows(0)], side_in.at[rows(0)], link_send.at[3], link_recv.at[3], beside))
    landed(near_in.at[3], near_recv.at[3])
    landed(far_in.at[rows(0)], link_recv.at[0])
    landed(side_in.at[rows(1)], link_recv.at[1])
    landed(far_in.at[rows(1)], link_recv.at[2])
    landed(side_in.at[rows(0)], link_recv.at[3])
    chunk = 64

    def body(i, _):
        r = pl.ds(pl.multiple_of(i * chunk, chunk), chunk)
        f32 = jnp.float32
        own[3, r, :] = (
            own[3, r, :]
            + near_in[3, r, :].astype(f32)
            + (far_in[r, :].astype(f32) + side_in[r, :].astype(f32))
        )
        return 0

    lax.fori_loop(0, tokens // chunk, body, 0)
    save = pltpu.make_async_copy(own.at[3], out, out_sem)
    save.start()
    for copy in copies:
        copy.wait_send()
    save.wait()


def add_rows(dst, own, near_in, k, start, count, extra=None, extra_start=0):
    chunk = 64

    def body(i, _):
        at = start + i * chunk
        r = pl.ds(pl.multiple_of(at, chunk), chunk)
        value = own[k, r, :] + near_in[k, r, :].astype(jnp.float32)
        if extra is not None:
            value += extra[pl.ds(pl.multiple_of(at - extra_start, chunk), chunk), :].astype(jnp.float32)
        dst[r, :] = value.astype(dst.dtype)
        return 0

    lax.fori_loop(0, count // chunk, body, 0)


def team_sum(lefts, rights, collective_id):
    pairs = len(lefts)
    _, tokens, inner = lefts[0].shape
    feats = rights[0].shape[1] // 2
    bf, f32 = jnp.bfloat16, jnp.float32
    any_spec = pl.BlockSpec(memory_space=pl.ANY)
    half = tokens // 2
    return pl.pallas_call(
        functools.partial(team_sum_kernel, pairs),
        out_shape=jax.ShapeDtypeStruct((tokens, feats), f32),
        in_specs=[any_spec] * (2 * pairs),
        out_specs=any_spec,
        scratch_shapes=[pltpu.VMEM((4, tokens, inner), bf)] * pairs
        + [pltpu.VMEM((inner, 2 * feats), bf)] * pairs
        + [
            pltpu.VMEM((4, tokens, feats), f32),
            pltpu.VMEM((4, tokens, feats), bf),
            pltpu.VMEM((4, tokens, feats), bf),
            pltpu.VMEM((tokens, feats), bf),
            pltpu.VMEM((half, feats), bf),
            pltpu.VMEM((half, feats), bf),
            pltpu.VMEM((tokens, feats), bf),
            pltpu.VMEM((tokens, feats), bf),
            pltpu.VMEM((tokens, feats), bf),
            pltpu.VMEM((tokens, feats), bf),
            pltpu.SemaphoreType.DMA((pairs, 2)),
            pltpu.SemaphoreType.DMA((4,)),
            pltpu.SemaphoreType.DMA((4,)),
            pltpu.SemaphoreType.DMA((2,)),
            pltpu.SemaphoreType.DMA((2,)),
            pltpu.SemaphoreType.DMA((4,)),
            pltpu.SemaphoreType.DMA((4,)),
            pltpu.SemaphoreType.DMA,
        ],
        compiler_params=pltpu.CompilerParams(
            collective_id=collective_id, has_side_effects=True, vmem_limit_bytes=48 * 2**20
        ),
        cost_estimate=pl.CostEstimate(
            flops=2 * 8 * tokens * feats * inner * pairs, bytes_accessed=30 * 2**20, transcendentals=0
        ),
        name="team_sum%d" % pairs,
    )(*lefts, *rights)


def weights_kernel(
    wq, wo, out_q, out_o, held_q, held_o, line_send, line_recv, own_sem, near_send, far_send, recv,
):
    b, y, z = me()
    c = lax.rem(b, 2)
    sib, far = xor(b, 1), xor(b, 2)
    far_sib = xor(far, 1)
    peers = [place(b, y, lax.rem(z + d, 4)) for d in (1, 2, 3)]
    team = [place(sib, y, z), place(far, y, z), place(far_sib, y, z)]
    greet(peers + team)
    rows_q, rows_o = wq.shape[0] // 4, wo.shape[0] // 4
    mine = (
        wq.at[pl.ds(pl.multiple_of(b * rows_q, rows_q), rows_q)],
        wo.at[pl.ds(pl.multiple_of(b * rows_o, rows_o), rows_o)],
    )
    held, outs = (held_q, held_o), (out_q, out_o)
    counts = (rows_q, rows_o)
    copies = []
    for w in (0, 1):
        for d in (0, 2, 1):
            copies.append(
                send(mine[w], held[w].at[z], line_send.at[w, d], line_recv.at[w, z], peers[d])
            )
        pltpu.make_async_copy(mine[w], held[w].at[z], own_sem.at[w]).start()
    waits = []
    for w in (0, 1):
        for d in (0, 1, 3, 2):
            block = lax.rem(z + d, 4)
            src = held[w].at[block]
            if d == 0:
                pltpu.make_async_copy(mine[w], src, own_sem.at[w]).wait()
            else:
                landed(src, line_recv.at[w, block])
            owner = lax.div(block, jnp.int32(2))
            slot = lax.rem(block + y, 2)
            dst = outs[w].at[slot, pl.ds(pl.multiple_of(b * counts[w], counts[w]), counts[w])]
            arrival = recv.at[w, slot, b]

            @pl.when(owner == c)
            def _(src=src, dst=dst, arrival=arrival, w=w, d=d):
                pltpu.make_async_copy(src, dst, arrival).start()
                send(src, dst, far_send.at[w, d], arrival, place(far, y, z))

            @pl.when(owner != c)
            def _(src=src, dst=dst, arrival=arrival, w=w, d=d):
                send(src, dst, near_send.at[w, d], arrival, place(sib, y, z))
                send(src, dst, far_send.at[w, d], arrival, place(far_sib, y, z))

            waits.append((w, d, src, owner))
    for w in (0, 1):
        for block in (0, 1):
            for q in range(4):
                ref = outs[w].at[block, pl.ds(q * counts[w], counts[w])]
                landed(ref, recv.at[w, block, q])
    for copy in copies:
        copy.wait_send()
    for w, d, src, owner in waits:
        pltpu.make_async_copy(src, src, far_send.at[w, d]).wait()

        @pl.when(owner != c)
        def _(src=src, w=w, d=d):
            pltpu.make_async_copy(src, src, near_send.at[w, d]).wait()


def gather_weights(w_qkv, w_out):
    any_spec = pl.BlockSpec(memory_space=pl.ANY)
    q, o = w_qkv.shape, w_out.shape
    dma = pltpu.SemaphoreType.DMA
    return pl.pallas_call(
        weights_kernel,
        out_shape=(
            jax.ShapeDtypeStruct((2, *q), w_qkv.dtype),
            jax.ShapeDtypeStruct((2, *o), w_out.dtype),
        ),
        in_specs=[any_spec] * 2,
        out_specs=(any_spec,) * 2,
        scratch_shapes=[
            pltpu.VMEM((4, q[0] // 4, q[1]), w_qkv.dtype),
            pltpu.VMEM((4, o[0] // 4, o[1]), w_out.dtype),
            dma((2, 3)),
            dma((2, 4)),
            dma((2,)),
            dma((2, 4)),
            dma((2, 4)),
            dma((2, 2, 4)),
        ],
        compiler_params=pltpu.CompilerParams(
            collective_id=3, has_side_effects=True, vmem_limit_bytes=8 * 2**20
        ),
        cost_estimate=pl.CostEstimate(flops=0, bytes_accessed=10 * 2**20, transcendentals=0),
        name="gather_weights",
    )(w_qkv, w_out)


def weight_sums_kernel(
    gq, go, out_q, out_o, got_q, got_o, line_q, line_o, sum_q, sum_o, all_q, all_o, res_q, res_o,
    part_send, part_recv, line_send, line_recv, all_send, all_recv, out_sem,
):
    b, y, z = me()
    c, x = lax.rem(b, 2), lax.div(b, jnp.int32(2))
    peers = [place(b, y, lax.rem(z + d, 4)) for d in (1, 2, 3)]
    team = [place(xor(b, 1), y, z), place(xor(b, 2), y, z), place(xor(xor(b, 2), 1), y, z)]
    greet(peers + team)
    f32 = jnp.float32
    rows = (gq.shape[1] // 4, go.shape[1] // 4)
    parts, got, line, sums, full, res, outs = (
        (gq, go), (got_q, got_o), (line_q, line_o), (sum_q, sum_o), (all_q, all_o), (res_q, res_o), (out_q, out_o),
    )
    targets = [b, xor(b, 1), xor(b, 2), xor(xor(b, 2), 1)]
    copies = []
    for w in (0, 1):
        for t in (3, 2, 1, 0):
            q = targets[t]
            for k in (0, 1):
                src = parts[w].at[k, pl.ds(pl.multiple_of(q * rows[w], rows[w]), rows[w])]
                block = 2 * c + (y if k == 0 else 1 - y)
                dst = got[w].at[block, x]
                arrival = part_recv.at[w, block, x]
                if t == 0:
                    pltpu.make_async_copy(src, dst, arrival).start()
                else:
                    copies.append(send(src, dst, part_send.at[w, t, k], arrival, place(q, y, z)))
    for w in (0, 1):
        for d in (2, 1, 3, 0):
            block = lax.rem(z + d, 4)
            for k in (0, 1):
                landed(got[w].at[block, k], part_recv.at[w, block, k])
            total = got[w][block, 0].astype(f32) + got[w][block, 1].astype(f32)
            if d == 0:
                res[w][...] = total
            else:
                sums[w][d] = total.astype(sums[w].dtype)
                copies.append(
                    send(
                        sums[w].at[d],
                        line[w].at[z],
                        line_send.at[w, d],
                        line_recv.at[w, z],
                        place(b, y, block),
                    )
                )
    for w in (0, 1):
        total = res[w][...]
        for d in (1, 3, 2):
            block = lax.rem(z + d, 4)
            landed(line[w].at[block], line_recv.at[w, block])
            total += line[w][block].astype(f32)
        full[w][b] = total.astype(full[w].dtype)
        for t in (3, 2, 1):
            copies.append(
                send(
                    full[w].at[b], full[w].at[b], all_send.at[w, t], all_recv.at[w, b], place(targets[t], y, z)
                )
            )
    for w in (0, 1):
        for t in (0, 1, 2, 3):
            q = targets[t]
            if t > 0:
                landed(full[w].at[q], all_recv.at[w, q])
            res[w][...] = full[w][q].astype(f32)
            save = pltpu.make_async_copy(
                res[w], outs[w].at[pl.ds(pl.multiple_of(q * rows[w], rows[w]), rows[w])], out_sem
            )
            save.start()
            save.wait()
    for copy in copies:
        copy.wait_send()


def sum_weights(grad_q, grad_o):
    any_spec = pl.BlockSpec(memory_space=pl.ANY)
    bf, f32 = jnp.bfloat16, jnp.float32
    q = (grad_q.shape[1] // 4, grad_q.shape[2])
    o = (grad_o.shape[1] // 4, grad_o.shape[2])
    dma = pltpu.SemaphoreType.DMA
    return pl.pallas_call(
        weight_sums_kernel,
        out_shape=(
            jax.ShapeDtypeStruct(grad_q.shape[1:], f32),
            jax.ShapeDtypeStruct(grad_o.shape[1:], f32),
        ),
        in_specs=[any_spec] * 2,
        out_specs=(any_spec,) * 2,
        scratch_shapes=[
            pltpu.VMEM((4, 2, *q), bf),
            pltpu.VMEM((4, 2, *o), bf),
            pltpu.VMEM((4, *q), bf),
            pltpu.VMEM((4, *o), bf),
            pltpu.VMEM((4, *q), bf),
            pltpu.VMEM((4, *o), bf),
            pltpu.VMEM((4, *q), bf),
            pltpu.VMEM((4, *o), bf),
            pltpu.VMEM(q, f32),
            pltpu.VMEM(o, f32),
            dma((2, 4, 2)),
            dma((2, 4, 2)),
            dma((2, 4)),
            dma((2, 4)),
            dma((2, 4)),
            dma((2, 4)),
            dma,
        ],
        compiler_params=pltpu.CompilerParams(
            collective_id=4, has_side_effects=True, vmem_limit_bytes=16 * 2**20
        ),
        cost_estimate=pl.CostEstimate(flops=0, bytes_accessed=10 * 2**20, transcendentals=0),
        name="sum_weights",
    )(grad_q, grad_o)


def gains_kernel(part, out, line, team, total, line_send, line_recv, team_send, team_recv):
    b, y, z = me()
    peers = [place(b, y, lax.rem(z + d, 4)) for d in (1, 2, 3)]
    mates = [place(lax.rem(b + d, 4), y, z) for d in (1, 2, 3)]
    greet(peers + mates)
    copies = []
    for d in range(3):
        copies.append(send(part, line.at[z], line_send.at[d], line_recv.at[z], peers[d]))
    line[z] = part[...]
    for d in (1, 2, 3):
        block = lax.rem(z + d, 4)
        landed(line.at[block], line_recv.at[block])
    value = (line[0] + line[1]) + (line[2] + line[3])
    total[...] = value
    team[b] = value
    for d in range(3):
        copies.append(send(total, team.at[b], team_send.at[d], team_recv.at[b], mates[d]))
    for d in (1, 2, 3):
        mate = lax.rem(b + d, 4)
        landed(team.at[mate], team_recv.at[mate])
    out[...] = (team[0] + team[1]) + (team[2] + team[3])
    for copy in copies:
        copy.wait_send()


def sum_gains(part):
    spec = pl.BlockSpec(memory_space=pltpu.VMEM)
    dma = pltpu.SemaphoreType.DMA
    return pl.pallas_call(
        gains_kernel,
        out_shape=jax.ShapeDtypeStruct(part.shape, part.dtype),
        in_specs=[spec],
        out_specs=spec,
        scratch_shapes=[
            pltpu.VMEM((4, *part.shape), part.dtype),
            pltpu.VMEM((4, *part.shape), part.dtype),
            pltpu.VMEM(part.shape, part.dtype),
            dma((3,)),
            dma((4,)),
            dma((3,)),
            dma((4,)),
        ],
        compiler_params=pltpu.CompilerParams(collective_id=5, has_side_effects=True),
        name="sum_gains",
    )(part)


def swap_row(tensor):
    return lax.ppermute(tensor, "row", [(0, 1), (1, 0)])


def swap_core(tensor):
    return lax.ppermute(tensor, "batch", [(0, 1), (1, 0), (2, 3), (3, 2)])


def swap_chip(tensor):
    return lax.ppermute(tensor, "batch", [(0, 2), (2, 0), (1, 3), (3, 1)])


def both_rows(values):
    return values + swap_row(values)


def fast_norm_forward(values, gain_vec):
    totals = both_rows(jnp.sum(values * values, axis=1))
    inverse = lax.rsqrt(totals / D + EPS)[:, None]
    normed = values * inverse
    return (normed, inverse, (normed * gain_vec).astype(jnp.bfloat16))


def fast_norm_backward(upstream, grad_hidden, normed, inverse, gain_vec):
    scaled = grad_hidden * gain_vec
    totals = both_rows(jnp.sum(scaled * normed, axis=1))
    centre = (totals / D)[:, None]
    return (upstream + inverse * (scaled - normed * centre), jnp.sum(grad_hidden * normed, axis=0))


def fast_shards(
    inputs,
    segments,
    positions,
    gain_attn,
    gain_mlp,
    w_qkv,
    w_out,
    w_gate,
    w_up,
    w_down,
    grad_output,
):
    bf = jnp.bfloat16
    f32 = jnp.float32
    b, y, z = me()
    seq_len = segments.shape[1]
    tokens, feats = inputs.shape
    query_cols = w_out.shape[0]
    block_cols = w_qkv.shape[1]
    head_size = block_cols - query_cols - (block_cols - query_cols) // 2
    group_heads = query_cols // head_size
    score_scale = 1.0 / math.sqrt(head_size)
    ff_cols = w_gate.shape[1]
    part = ff_cols // 8

    def eighth(index):
        gate_up_part = jnp.stack(
            [
                lax.dynamic_slice_in_dim(w_gate, index * part, part, 1).T,
                lax.dynamic_slice_in_dim(w_up, index * part, part, 1).T,
            ]
        )
        return gate_up_part, lax.dynamic_slice_in_dim(w_down, index * part, part, 0)

    gate_up_mine, down_mine = eighth(2 * b + y)
    gate_up_sent, down_sent = eighth(2 * b + 1 - y)
    gate_up_w = jnp.concatenate([gate_up_mine, swap_row(gate_up_sent)], axis=2)
    down_w = jnp.concatenate([down_mine, swap_row(down_sent)], axis=1)
    gate_up_w = lax.all_gather(gate_up_w, "col", axis=1, tiled=True)
    down_w = lax.all_gather(down_w, "col", axis=0, tiled=True)
    gate_w, up_w = gate_up_w[0], gate_up_w[1]

    normed_one, inverse_one, hidden_one = fast_norm_forward(inputs, gain_attn)
    wq, wo = gather_weights(w_qkv, w_out)
    wide_one = jnp.concatenate([hidden_one, swap_core(hidden_one)], axis=0)

    grad_b = grad_output.astype(bf)
    grad_chip, grad_row = swap_chip(grad_b), swap_row(grad_b)
    grad_corner = swap_chip(grad_row)
    grad_sibs = swap_core(jnp.stack([grad_b, grad_row, grad_chip, grad_corner]))
    wide_grad = jnp.concatenate(
        [
            jnp.concatenate([grad_b, grad_row], axis=1),
            jnp.concatenate([grad_sibs[0], grad_sibs[1]], axis=1),
            jnp.concatenate([grad_chip, grad_corner], axis=1),
            jnp.concatenate([grad_sibs[2], grad_sibs[3]], axis=1),
        ],
        axis=0,
    )

    places = jnp.stack([segments, positions], axis=1)
    their_places = swap_row(places)
    places = jnp.where(
        y == 0,
        jnp.concatenate([places, their_places], axis=0),
        jnp.concatenate([their_places, places], axis=0),
    )
    places = lax.dynamic_index_in_dim(places, z, 0, keepdims=False)
    places = jnp.stack([places, swap_core(places)])
    seg, pos = places[:, 0], places[:, 1]
    cosine_table, sine_table = rope_tables(pos, head_size)

    sent = matmul(wide_one, wq[1]).astype(bf)
    qkv_local = matmul(wide_one, wq[0]) + swap_row(sent).astype(f32)
    seq_count = 2
    queries = qkv_local[:, :query_cols].reshape(seq_count, seq_len, group_heads, head_size)
    key_part = qkv_local[:, query_cols : query_cols + head_size].reshape(
        seq_count, seq_len, head_size
    )
    value_matrix = (
        qkv_local[:, query_cols + head_size :].reshape(seq_count, seq_len, head_size).astype(bf)
    )
    rotary_queries = rotate(queries, cosine_table[:, :, None, :], sine_table[:, :, None, :]).astype(
        bf
    )
    rotary_keys = rotate(key_part, cosine_table, sine_table).astype(bf)
    attention_output, log_total = attend_forward(
        rotary_queries, rotary_keys, value_matrix, seg, score_scale
    )
    attended = attention_output.reshape(2 * tokens, query_cols)
    attended_theirs = swap_row(attended)
    out_partial = matmul(attended, wo[0]) + matmul(attended_theirs, wo[1])
    mixed_in = inputs + (out_partial[:tokens] + swap_core(out_partial[tokens:]))
    normed_two, inverse_two, hidden_two = fast_norm_forward(mixed_in, gain_mlp)

    wide_two, gate_vals, up_vals, activated = gate_up(hidden_two, gate_w, up_w)
    wide_two = wide_two.reshape(4 * tokens, 2 * feats)
    flat_act = activated.reshape(4 * tokens, 4 * part)

    grad_w_down = left_t(flat_act, wide_grad).astype(bf)
    grad_act = right_t(wide_grad, down_w).reshape(gate_vals.shape)
    gate_sigmoid = jax.nn.sigmoid(gate_vals)
    grad_gate = (
        grad_act * up_vals * gate_sigmoid * (1.0 + gate_vals * (1.0 - gate_sigmoid))
    ).astype(bf)
    grad_up = (grad_act * gate_vals * gate_sigmoid).astype(bf)
    grad_hidden_two = team_sum((grad_gate, grad_up), (gate_w, up_w), 2)
    flat_grads = jnp.concatenate([grad_gate, grad_up], axis=2).reshape(4 * tokens, 8 * part)
    grad_w_gate_up = left_t(flat_grads, wide_two).astype(bf).reshape(2, 4 * part, 2 * feats)
    grad_mixed, grad_gain_mlp = fast_norm_backward(
        grad_output, grad_hidden_two, normed_two, inverse_two, gain_mlp
    )

    grad_mixed_b = grad_mixed.astype(bf)
    wide_mixed = jnp.concatenate([grad_mixed_b, swap_core(grad_mixed_b)], axis=0)
    sent = right_t(wide_mixed, wo[1]).astype(bf)
    attention_output_gradient = (
        (right_t(wide_mixed, wo[0]) + swap_row(sent).astype(f32))
        .astype(bf)
        .reshape(seq_count, seq_len, group_heads, head_size)
    )
    grad_qrot, grad_krot, grad_value = attend_backward(
        rotary_queries,
        rotary_keys,
        value_matrix,
        seg,
        log_total,
        attention_output_gradient,
        score_scale,
    )
    grad_query = rotate(grad_qrot, cosine_table[:, :, None, :], -sine_table[:, :, None, :]).reshape(
        2 * tokens, query_cols
    )
    grad_key = rotate(grad_krot, cosine_table, -sine_table).reshape(2 * tokens, head_size)
    grad_qkv = jnp.concatenate(
        [grad_query, grad_key, grad_value.reshape(2 * tokens, head_size)], axis=1
    ).astype(bf)
    grad_qkv_theirs = swap_row(grad_qkv)
    one_partial = right_t(grad_qkv, wq[0]) + right_t(grad_qkv_theirs, wq[1])
    grad_hidden_one = one_partial[:tokens] + swap_core(one_partial[tokens:])
    grad_inputs, grad_gain_attn = fast_norm_backward(
        grad_mixed, grad_hidden_one, normed_one, inverse_one, gain_attn
    )
    gains = sum_gains(jnp.stack([grad_gain_attn, grad_gain_mlp]))

    grad_wq = jnp.stack([left_t(wide_one, grad_qkv), left_t(wide_one, grad_qkv_theirs)]).astype(bf)
    grad_wo = jnp.stack([left_t(attended, wide_mixed), left_t(attended_theirs, wide_mixed)]).astype(bf)
    grad_w_qkv, grad_w_out = sum_weights(grad_wq, grad_wo)

    result = mixed_in + team_sum((activated,), (down_w,), 6)

    def assemble(summed):
        pair = jnp.stack([summed[..., :feats], swap_row(summed[..., feats:])], axis=-3)
        pair = jnp.where(y == 0, pair, jnp.flip(pair, axis=-3))
        sides = jnp.stack([pair, swap_chip(pair)], axis=0)
        both = jnp.stack([sides, swap_core(sides)], axis=1)
        first = jnp.where(lax.rem(b, 2) == 0, both, jnp.flip(both, axis=1))
        whole = jnp.where(b < 2, first, jnp.flip(first, axis=0))
        return whole

    down_sum = lax.psum_scatter(grad_w_down, "col", scatter_dimension=0, tiled=True)
    grad_w_down = assemble(down_sum).reshape(ff_cols, feats).astype(f32)
    gate_up_sum = lax.psum_scatter(grad_w_gate_up, "col", scatter_dimension=1, tiled=True)
    grads = jnp.moveaxis(assemble(gate_up_sum), 2, 0).reshape(2, ff_cols, feats)
    grad_w_gate = grads[0].T.astype(f32)
    grad_w_up = grads[1].T.astype(f32)
    return (
        result,
        grad_inputs,
        gains[0],
        gains[1],
        grad_w_qkv,
        grad_w_out,
        grad_w_gate,
        grad_w_up,
        grad_w_down,
    )


def solution(mesh):
    shape = mesh.shape
    team = shape["batch"] == 4 and shape["row"] == 2 and shape["col"] == 4
    return jax.shard_map(
        fast_shards if team else shards,
        mesh=mesh,
        in_specs=(
            P(("batch", "col"), "row"),
            P(("batch", "row"), None),
            P(("batch", "row"), None),
            P("row"),
            P("row"),
            P("row", "col"),
            P("col", "row"),
            P("row", "col"),
            P("row", "col"),
            P("col", "row"),
            P(("batch", "col"), "row"),
        ),
        out_specs=(
            P(("batch", "col"), "row"),
            P(("batch", "col"), "row"),
            P("row"),
            P("row"),
            P("row", "col"),
            P("col", "row"),
            P("row", "col"),
            P("row", "col"),
            P("col", "row"),
        ),
        check_vma=False,
    )
```
